32 devices in a mesh: grp: 4 (over x, core), bn: 8 (over z, y).
Axes of the slice: x: 2, y: 2, z: 4, core: 2. Of those that a mesh axis runs over, the one named last changes fastest.
Arguments:
- images: bfloat16 [16, 32, 64, 1024], P('grp', 'bn'), parts along dimension 0, may hold values from -64 to 64
- w_reduce: bfloat16 [1024, 256], replicated, may hold values from -0.1875 to 0.1875
- w_spatial: bfloat16 [3, 3, 256, 256], replicated, may hold values from -0.125 to 0.125
- w_expand: bfloat16 [256, 1024], replicated, may hold values from -0.375 to 0.375
- gain_first: float32 [256], replicated, may hold values from 0.25 to 1.75
- shift_first: float32 [256], replicated, may hold values from -3 to 3
- gain_middle: float32 [256], replicated, may hold values from 0.25 to 1.75
- shift_middle: float32 [256], replicated, may hold values from -3 to 3
- gain_last: float32 [1024], replicated, may hold values from 0.25 to 1.75
- shift_last: float32 [1024], replicated, may hold values from -3 to 3
Outputs:
- block_out: bfloat16 [16, 32, 64, 1024], P('grp', 'bn'), parts along dimension 0
The draws below stay inside these ranges and needn't reach their ends.
There are 4 independent parts, one for each index of `grp`. The reference program is written for one: setup_inputs(seed, part) draws one part's arguments, and reference() takes and returns one part's arrays. A program takes and returns all parts, laid end to end along the dimension named above; an argument that names none is the same for every part. Nothing has to cross between parts.
All inputs are finite; a program needn't handle non-finite values.
Results may differ from the reference program's by a relative error of at most 0.0034.
Values may be sent and summed in bfloat16 or wider, within the bound.
A program may use at most 64 MiB of HBM per device.

```python
import math
import jax
import jax.numpy as jnp
from jax import lax

CH = 1024
MID = 256
IMGS = 4
WID = 64
HGT = 32


def draw_images(key, part):
    keys = jax.random.split(key, 8)
    noise = jnp.clip(jax.random.normal(keys[0], (IMGS, HGT, WID, CH), jnp.float32), -4.0, 4.0)
    position = jnp.arange(HGT, dtype=jnp.float32) / max(HGT - 1, 1)
    jitter = jnp.exp(jax.random.uniform(keys[1], (IMGS, HGT), jnp.float32, 0.0, math.log(1.5)))
    offset = 0.5 * jnp.clip(jax.random.normal(keys[2], (IMGS, CH), jnp.float32), -3.0, 3.0)
    scale = jnp.power(3.0, position)[None, :] * jitter
    row_freq = jax.random.randint(keys[4], (IMGS, 3), 0, 2).astype(jnp.float32)
    col_freq = jax.random.randint(keys[5], (IMGS, 3), 1, 3).astype(jnp.float32)
    phases = jax.random.uniform(keys[6], (IMGS, 3), jnp.float32, 0.0, 2.0 * math.pi)
    amplitude = jnp.clip(jax.random.normal(keys[7], (IMGS, 3), jnp.float32), -3.0, 3.0)
    rows = jnp.arange(HGT, dtype=jnp.float32) / HGT
    cols = jnp.arange(WID, dtype=jnp.float32) / WID
    angles = 2.0 * math.pi * (row_freq[:, :, None, None] * rows[None, None, :, None] + col_freq[:, :, None, None] * cols[None, None, None, :]) + phases[:, :, None, None]
    waves = jnp.sum(amplitude[:, :, None, None] * jnp.cos(angles), axis=1)
    field = jnp.exp(0.7 * jnp.tanh(waves))
    values = (noise + offset[:, None, None, :]) * (scale[:, :, None] * field)[:, :, :, None]
    return values.astype(jnp.bfloat16)


def scatter_about(key, extent, scale, reach, held_as=jnp.bfloat16):
    array = jax.random.normal(key, extent, jnp.float32) * scale
    return jnp.minimum(jnp.maximum(array, -reach), reach).astype(held_as)


def setup_inputs(seed: int = 0, part: int = 0) -> dict:
    seeds = jax.random.split(jax.random.key(seed), 11)
    part_splits = jax.random.split(jax.random.fold_in(seeds[10], part), 11)
    images = draw_images(jax.random.fold_in(jax.random.fold_in(seeds[10], part), 71), part)
    w_reduce = scatter_about(seeds[1], (CH, MID), CH ** -0.5, 0.1875)
    w_spatial = scatter_about(seeds[2], (3, 3, MID, MID), (9 * MID) ** -0.5, 0.125)
    w_expand = scatter_about(seeds[3], (MID, CH), MID ** -0.5, 0.375)
    gain_first = jnp.clip(1.0 + 0.15 * jax.random.normal(seeds[4], (MID,), jnp.float32), 0.25, 1.75)
    shift_first = scatter_about(seeds[5], (MID,), 0.5, 3.0, jnp.float32)
    gain_middle = jnp.clip(1.0 + 0.15 * jax.random.normal(seeds[6], (MID,), jnp.float32), 0.25, 1.75)
    shift_middle = scatter_about(seeds[7], (MID,), 0.5, 3.0, jnp.float32)
    gain_last = jnp.clip(1.0 + 0.15 * jax.random.normal(seeds[8], (CH,), jnp.float32), 0.25, 1.75)
    shift_last = scatter_about(seeds[9], (CH,), 0.5, 3.0, jnp.float32)
    return {"images": images, "w_reduce": w_reduce, "w_spatial": w_spatial, "w_expand": w_expand, "gain_first": gain_first, "shift_first": shift_first, "gain_middle": gain_middle, "shift_middle": shift_middle, "gain_last": gain_last, "shift_last": shift_last}


epsilon = 1e-05

def normalize(values, gain, shift):
    population = values.shape[0] * values.shape[1] * values.shape[2]
    average = lax.optimization_barrier(jnp.sum(values, axis=(0, 1, 2))) / population
    centred = values - average
    spread = lax.optimization_barrier(jnp.sum(centred * centred, axis=(0, 1, 2))) / population
    return centred * (gain * lax.rsqrt(spread + epsilon)) + shift

def pointwise(inputs, weight):
    flat = inputs.reshape(-1, inputs.shape[-1])
    product = jnp.dot(flat, weight, preferred_element_type=jnp.float32)
    return product.reshape(inputs.shape[:-1] + (weight.shape[1],))

def reference(images, w_reduce, w_spatial, w_expand, gain_first, shift_first, gain_middle, shift_middle, gain_last, shift_last):
    first = pointwise(images, w_reduce)
    hidden_first = jax.nn.relu(normalize(first, gain_first, shift_first)).astype(jnp.bfloat16)
    middle = lax.conv_general_dilated(hidden_first, w_spatial, (1, 1), 'SAME', dimension_numbers=('NHWC', 'HWIO', 'NHWC'), preferred_element_type=jnp.float32)
    hidden_middle = jax.nn.relu(normalize(middle, gain_middle, shift_middle)).astype(jnp.bfloat16)
    last = pointwise(hidden_middle, w_expand)
    return jax.nn.relu(normalize(last, gain_last, shift_last) + images.astype(jnp.float32)).astype(jnp.bfloat16)
```

```python
import functools

import jax
import jax.numpy as jnp
from jax import lax
from jax.experimental import pallas as pl
from jax.experimental.pallas import tpu as pltpu
from jax.sharding import PartitionSpec as P

epsilon = 1e-05
AXIS = "bn"
f32 = jnp.float32
bf16 = jnp.bfloat16
PIVOT_ROWS = 16


def dot(a, b):
    return jnp.dot(a, b, preferred_element_type=f32)


def kernel(
    n, imgs, rows, wid,
    images, w_reduce, w_spatial, w_expand, g1, b1, g2, b2, g3,
    h_out, coef,
    xbuf, wr, ws, we, g1v, b1v, g2v, b2v, g3v,
    first, xcat, middle, hm, up_src, down_src, up_dst, down_dst,
    st1, st2, st3,
    load_sem, out_sem, halo_send, halo_recv, st_send, st_recv,
):
    me = lax.axis_index(AXIS)
    cells = imgs * wid
    count = rows * cells
    mid = wr.shape[1]

    barrier = pltpu.get_barrier_semaphore()
    for k in range(1, n):
        pl.semaphore_signal(
            barrier, inc=1, device_id={AXIS: lax.rem(me + k, n)},
            device_id_type=pl.DeviceIdType.MESH,
        )

    edges = [0] + ([rows - 1] if rows > 1 else [])
    order = edges + [r for r in range(rows) if r not in edges]
    slot = iter(range(load_sem.shape[0]))

    def load(src, dst):
        copy = pltpu.make_async_copy(src, dst, load_sem.at[next(slot)])
        copy.start()
        return copy

    wr_copy = load(w_reduce, wr)
    x_copies = {r: load(images.at[:, r], xbuf.at[r]) for r in order}
    first_vec = [load(g1, g1v), load(b1, b1v)]
    ws_copy = load(w_spatial, ws)
    mid_vec = [load(g2, g2v), load(b2, b2v)]
    we_copy = load(w_expand, we)
    last_vec = [load(g3, g3v)]

    has_up = me > 0
    has_down = me < n - 1
    up_copy = pltpu.make_async_remote_copy(
        src_ref=up_src, dst_ref=up_dst, send_sem=halo_send.at[0], recv_sem=halo_recv.at[0],
        device_id={AXIS: lax.rem(me + n - 1, n)}, device_id_type=pl.DeviceIdType.MESH,
    )
    down_copy = pltpu.make_async_remote_copy(
        src_ref=down_src, dst_ref=down_dst, send_sem=halo_send.at[1], recv_sem=halo_recv.at[1],
        device_id={AXIS: lax.rem(me + 1, n)}, device_id_type=pl.DeviceIdType.MESH,
    )

    def exchange_start(index, buf):
        copies = []
        for k in range(1, n):
            copy = pltpu.make_async_remote_copy(
                src_ref=buf.at[0], dst_ref=buf.at[k],
                send_sem=st_send.at[index, k - 1], recv_sem=st_recv.at[index, k - 1],
                device_id={AXIS: lax.rem(me + k, n)}, device_id_type=pl.DeviceIdType.MESH,
            )
            copy.start()
            copies.append(copy)
        return copies

    def exchange_end(copies, buf):
        for copy in copies:
            copy.wait_recv()
        values = buf[...]
        total = jnp.sum(values, axis=0)
        average = total[0:1] / n
        gap = values[:, 0:1, :] - average
        spread = (total[1:2] + count * jnp.sum(gap * gap, axis=0)) / (n * count)
        return average, spread

    wr_copy.wait()
    total = jnp.zeros((1, mid), f32)
    for r in order:
        x_copies[r].wait()
        value = dot(xbuf[r].reshape(cells, xbuf.shape[-1]), wr[...])
        first[r] = value
        part = jnp.sum(value, axis=0, keepdims=True)
        total = total + part
        for row, src in ((0, up_src), (rows - 1, down_src)):
            if r == row:
                pivot = (part / cells).astype(bf16)
                src[pl.ds(0, cells), :] = (value - pivot.astype(f32)).astype(bf16)
                src[pl.ds(cells, PIVOT_ROWS), :] = jnp.broadcast_to(pivot, (PIVOT_ROWS, mid))
    average = total / count
    second = jnp.zeros((1, mid), f32)
    for r in range(rows):
        gap = first[r] - average
        second = second + jnp.sum(gap * gap, axis=0, keepdims=True)
    st1[0, 0:1, :] = average
    st1[0, 1:2, :] = second

    pl.semaphore_wait(barrier, n - 1)
    copies1 = exchange_start(0, st1)

    @pl.when(has_up)
    def _():
        up_copy.start()

    @pl.when(has_down)
    def _():
        down_copy.start()

    for copy in first_vec:
        copy.wait()
    average, spread = exchange_end(copies1, st1)
    scale = g1v[...] * lax.rsqrt(spread + epsilon)
    shift = b1v[...]
    column = lax.rem(lax.broadcasted_iota(jnp.int32, (cells, mid), 0), wid)

    def fill(r, value):
        h = jnp.maximum((value - average) * scale + shift, 0.0)
        xcat[r, :, pl.ds(mid, mid)] = h.astype(bf16)
        before = jnp.where(column == 0, 0.0, pltpu.roll(h, 1, 0))
        xcat[r, :, pl.ds(0, mid)] = before.astype(bf16)
        after = jnp.where(column == wid - 1, 0.0, pltpu.roll(h, cells - 1, 0))
        xcat[r, :, pl.ds(2 * mid, mid)] = after.astype(bf16)

    for r in range(rows):
        fill(r + 1, first[r])

    ws_copy.wait()
    for r in range(rows):
        acc = dot(xcat[r + 1], ws[1])
        if r > 0:
            acc = acc + dot(xcat[r], ws[0])
        if r < rows - 1:
            acc = acc + dot(xcat[r + 2], ws[2])
        middle[r] = acc

    def halo(src):
        return src[pl.ds(0, cells), :].astype(f32) + src[pl.ds(cells, 1), :].astype(f32)

    @pl.when(has_up)
    def _():
        down_copy.wait_recv()
        fill(0, halo(down_dst))
        middle[0] += dot(xcat[0], ws[0])

    @pl.when(has_down)
    def _():
        up_copy.wait_recv()
        fill(rows + 1, halo(up_dst))
        middle[rows - 1] += dot(xcat[rows + 1], ws[2])

    total = jnp.zeros((1, mid), f32)
    for r in range(rows):
        total = total + jnp.sum(middle[r], axis=0, keepdims=True)
    average = total / count
    second = jnp.zeros((1, mid), f32)
    for r in range(rows):
        gap = middle[r] - average
        second = second + jnp.sum(gap * gap, axis=0, keepdims=True)
    st2[0, 0:1, :] = average
    st2[0, 1:2, :] = second
    copies2 = exchange_start(1, st2)
    for copy in mid_vec + last_vec:
        copy.wait()
    we_copy.wait()
    average, spread = exchange_end(copies2, st2)
    scale = g2v[...] * lax.rsqrt(spread + epsilon)
    shift = b2v[...]
    out_copies = []
    total = jnp.zeros((1, mid), f32)
    for r in range(rows):
        h = jnp.maximum((middle[r] - average) * scale + shift, 0.0)
        total = total + jnp.sum(h, axis=0, keepdims=True)
        hm[r] = h.astype(bf16).reshape(imgs, wid, mid)
        copy = pltpu.make_async_copy(hm.at[r], h_out.at[:, r], out_sem.at[r])
        copy.start()
        out_copies.append(copy)

    pivot = dot((total / count).astype(bf16), we[...])
    one = jnp.zeros_like(pivot)
    two = jnp.zeros_like(pivot)
    for r in range(rows):
        gap = dot(hm[r].reshape(cells, mid), we[...]) - pivot
        one = one + jnp.sum(gap, axis=0, keepdims=True)
        two = two + jnp.sum(gap * gap, axis=0, keepdims=True)
    st3[0, 0:1, :] = pivot + one / count
    st3[0, 1:2, :] = two - one * (one / count)
    copies3 = exchange_start(2, st3)
    for copy in copies1 + copies2:
        copy.wait_send()

    @pl.when(has_up)
    def _():
        up_copy.wait_send()

    @pl.when(has_down)
    def _():
        down_copy.wait_send()

    for copy in out_copies:
        copy.wait()
    average, spread = exchange_end(copies3, st3)
    coef[0:1, :] = average
    coef[1:2, :] = g3v[...] * lax.rsqrt(spread + epsilon)
    for copy in copies3:
        copy.wait_send()


def body(images, w_reduce, w_spatial, w_expand, g1, b1, g2, b2, g3, b3):
    n = lax.axis_size(AXIS)
    imgs, rows, wid, ch = images.shape
    mid = w_reduce.shape[1]
    cells = imgs * wid
    any_spec = pl.BlockSpec(memory_space=pl.ANY)
    vec = lambda c: pltpu.VMEM((1, c), f32)
    rowvec = lambda v: v.reshape(1, v.shape[0])
    halo = pltpu.VMEM((cells + PIVOT_ROWS, mid), bf16)
    hidden, coef = pl.pallas_call(
        functools.partial(kernel, n, imgs, rows, wid),
        out_shape=(
            jax.ShapeDtypeStruct((imgs, rows, wid, mid), bf16),
            jax.ShapeDtypeStruct((2, ch), f32),
        ),
        in_specs=[any_spec] * 9,
        out_specs=(any_spec, pl.BlockSpec(memory_space=pltpu.VMEM)),
        scratch_shapes=[
            pltpu.VMEM((rows, imgs, wid, ch), bf16),
            pltpu.VMEM((ch, mid), bf16),
            pltpu.VMEM((3, 3 * mid, mid), bf16),
            pltpu.VMEM((mid, ch), bf16),
            vec(mid), vec(mid), vec(mid), vec(mid), vec(ch),
            pltpu.VMEM((rows, cells, mid), f32),
            pltpu.VMEM((rows + 2, cells, 3 * mid), bf16),
            pltpu.VMEM((rows, cells, mid), f32),
            pltpu.VMEM((rows, imgs, wid, mid), bf16),
            halo, halo, halo, halo,
            pltpu.VMEM((n, 2, mid), f32),
            pltpu.VMEM((n, 2, mid), f32),
            pltpu.VMEM((n, 2, ch), f32),
            pltpu.SemaphoreType.DMA((rows + 8,)),
            pltpu.SemaphoreType.DMA((rows,)),
            pltpu.SemaphoreType.DMA((2,)),
            pltpu.SemaphoreType.DMA((2,)),
            pltpu.SemaphoreType.DMA((3, n - 1)),
            pltpu.SemaphoreType.DMA((3, n - 1)),
        ],
        compiler_params=pltpu.CompilerParams(
            collective_id=0, has_side_effects=True, vmem_limit_bytes=32 * 1024 * 1024
        ),
        name="block_front",
    )(
        images, w_reduce, w_spatial.reshape(3, 3 * mid, mid), w_expand,
        rowvec(g1), rowvec(b1), rowvec(g2), rowvec(b2), rowvec(g3),
    )
    last = jnp.einsum("nhwc,cd->nhwd", hidden, w_expand, preferred_element_type=f32)
    summed = (last - coef[0]) * coef[1] + b3 + images.astype(f32)
    return jax.nn.relu(summed).astype(bf16)


def solution(mesh):
    placed = (P("grp", "bn", None, None), P(), P(), P(), P(), P(), P(), P(), P(), P())
    return jax.shard_map(
        body, mesh=mesh, in_specs=placed, out_specs=P("grp", "bn", None, None), check_vma=False
    )
```

```python
import functools

import jax
import jax.numpy as jnp
from jax import lax
from jax.experimental import pallas as pl
from jax.experimental.pallas import tpu as pltpu
from jax.sharding import PartitionSpec as P

epsilon = 1e-05
AXIS = "bn"
f32 = jnp.float32
bf16 = jnp.bfloat16
PIVOT_ROWS = 16
PIECES = 8


def dot(a, b):
    return jnp.dot(a, b, preferred_element_type=f32)


def flipped(me, k):
    bit, out = 1, me
    while bit <= k:
        if k & bit:
            out = out + bit * (1 - 2 * lax.rem(me // bit, 2))
        bit *= 2
    return out


def kernel(
    n, imgs, rows, wid, chunks,
    images, w_reduce, w_spatial, w_expand, g1, b1, g2, b2, g3,
    x_out, last_out, coef,
    wr, ws, we, g1v, b1v, g2v, b2v, g3v,
    first, xcat, middle, up_src, down_src, up_dst, down_dst,
    st1, st2, st3,
    load_sem, halo_send, halo_recv, st_send, st_recv,
):
    me = lax.axis_index(AXIS)
    cells = imgs * wid
    sizes = [c * wid for c in chunks]
    starts = [sum(sizes[:c]) for c in range(len(sizes))]
    chunks = len(sizes)
    count = rows * cells
    mid = wr.shape[1]
    ch = wr.shape[0]
    paired = n & (n - 1) == 0

    def peer(k):
        return flipped(me, k) if paired else lax.rem(me + k, n)

    hops = list(range(n - 1, 0, -1))
    barrier = pltpu.get_barrier_semaphore()
    for k in hops:
        pl.semaphore_signal(
            barrier, inc=1, device_id={AXIS: peer(k)}, device_id_type=pl.DeviceIdType.MESH
        )

    edges = [0] + ([rows - 1] if rows > 1 else [])
    inner = [r for r in range(rows) if r not in edges]
    slot = iter(range(load_sem.shape[0]))

    def load(src, dst):
        copy = pltpu.make_async_copy(src, dst, load_sem.at[next(slot)])
        copy.start()
        return copy

    wr_copy = load(w_reduce, wr)
    x_copies = {r: load(images.at[:, r], x_out.at[:, r]) for r in edges + inner}
    first_vec = [load(g1, g1v), load(b1, b1v)]
    ws_copy = load(w_spatial, ws)
    mid_vec = [load(g2, g2v), load(b2, b2v)]
    we_copy = load(w_expand, we)
    last_vec = [load(g3, g3v)]

    has_up = me > 0
    has_down = me < n - 1

    def span(c):
        begin = 0 if c == 0 else PIVOT_ROWS + starts[c]
        return pl.ds(begin, PIVOT_ROWS + starts[c] + sizes[c] - begin)

    def halo_copy(c, side):
        src, dst, to = ((up_src, up_dst, n - 1), (down_src, down_dst, 1))[side]
        return pltpu.make_async_remote_copy(
            src_ref=src.at[span(c)], dst_ref=dst.at[span(c)],
            send_sem=halo_send.at[side, c], recv_sem=halo_recv.at[side, c],
            device_id={AXIS: lax.rem(me + to, n)}, device_id_type=pl.DeviceIdType.MESH,
        )

    up_copies = [halo_copy(c, 0) for c in range(chunks)]
    down_copies = [halo_copy(c, 1) for c in range(chunks)]

    def exchange_start(index, buf):
        copies = []
        for k in hops:
            copy = pltpu.make_async_remote_copy(
                src_ref=buf.at[0], dst_ref=buf.at[k],
                send_sem=st_send.at[index, k - 1], recv_sem=st_recv.at[index, k - 1],
                device_id={AXIS: peer(k)}, device_id_type=pl.DeviceIdType.MESH,
            )
            copy.start()
            copies.append(copy)
        return copies

    def exchange_end(copies, buf):
        for copy in copies:
            copy.wait_recv()
        values = buf[...]
        total = jnp.sum(values, axis=0)
        average = total[0:1] / n
        gap = values[:, 0:1, :] - average
        spread = (total[1:2] + count * jnp.sum(gap * gap, axis=0)) / (n * count)
        return average, spread

    def colsum(v):
        return jnp.sum(v, axis=0, keepdims=True)

    def pooled(buf, pivot, one, two):
        buf[0, 0:1, :] = pivot + one / count
        buf[0, 1:2, :] = two - one * (one / count)

    wr_copy.wait()
    pivot = None
    one = jnp.zeros((1, mid), f32)
    two = jnp.zeros((1, mid), f32)
    for r in edges + inner:
        x_copies[r].wait()
        value = dot(x_out[:, r].reshape(cells, ch), wr[...])
        first[r] = value
        if pivot is None:
            pivot = colsum(value) / cells
        gap = value - pivot
        one = one + colsum(gap)
        two = two + colsum(gap * gap)
        for row, src in ((0, up_src), (rows - 1, down_src)):
            if r == row:
                centre = (colsum(value) / cells).astype(bf16)
                sent = (value - centre.astype(f32)).astype(bf16)
                src[pl.ds(0, PIVOT_ROWS), :] = jnp.broadcast_to(centre, (PIVOT_ROWS, mid))
                src[pl.ds(PIVOT_ROWS, cells), :] = sent
    pooled(st1, pivot, one, two)

    pl.semaphore_wait(barrier, n - 1)
    copies1 = exchange_start(0, st1)
    for c in range(chunks):
        pl.when(has_up)(up_copies[c].start)
        pl.when(has_down)(down_copies[c].start)

    for copy in first_vec:
        copy.wait()
    average, spread = exchange_end(copies1, st1)
    scale = g1v[...] * lax.rsqrt(spread + epsilon)
    shift = b1v[...]

    def columns(size):
        shape = (size // wid, wid, mid)
        return lax.broadcasted_iota(jnp.int32, shape, 1).reshape(size, mid)

    def fill(r, start, value):
        size = value.shape[0]
        column = columns(size)
        h = jnp.maximum((value - average) * scale + shift, 0.0)
        here = pl.ds(start, size)
        xcat[r, here, pl.ds(mid, mid)] = h.astype(bf16)
        before = jnp.where(column == 0, 0.0, pltpu.roll(h, 1, 0))
        xcat[r, here, pl.ds(0, mid)] = before.astype(bf16)
        after = jnp.where(column == wid - 1, 0.0, pltpu.roll(h, size - 1, 0))
        xcat[r, here, pl.ds(2 * mid, mid)] = after.astype(bf16)

    for r in range(rows):
        fill(r + 1, 0, first[r])

    ws_copy.wait()
    for r in range(rows):
        acc = dot(xcat[r + 1], ws[1])
        if r > 0:
            acc = acc + dot(xcat[r], ws[0])
        if r < rows - 1:
            acc = acc + dot(xcat[r + 2], ws[2])
        middle[r] = acc

    based = inner or edges
    pivot = jnp.zeros((1, mid), f32)
    for r in based:
        pivot = pivot + colsum(middle[r])
    pivot = pivot / (len(based) * cells)
    one = jnp.zeros((1, mid), f32)
    two = jnp.zeros((1, mid), f32)
    for r in inner:
        gap = middle[r] - pivot
        one = one + colsum(gap)
        two = two + colsum(gap * gap)

    def add_halo(dst, c, padded_row, row, tap):
        value = dst[pl.ds(PIVOT_ROWS + starts[c], sizes[c]), :].astype(f32)
        fill(padded_row, starts[c], value + dst[pl.ds(0, 1), :].astype(f32))
        here = pl.ds(starts[c], sizes[c])
        middle[row, here, :] += dot(xcat[padded_row, here, :], ws[tap])

    for c in range(chunks):
        @pl.when(has_down)
        def _():
            up_copies[c].wait_recv()
            add_halo(up_dst, c, rows + 1, rows - 1, 2)

        @pl.when(has_up)
        def _():
            down_copies[c].wait_recv()
            add_halo(down_dst, c, 0, 0, 0)

        for r in edges:
            gap = middle[r, pl.ds(starts[c], sizes[c]), :] - pivot
            one = one + colsum(gap)
            two = two + colsum(gap * gap)

    pooled(st2, pivot, one, two)
    copies2 = exchange_start(1, st2)
    for copy in mid_vec + last_vec:
        copy.wait()
    we_copy.wait()
    for copy in copies1:
        copy.wait_send()
    for c in range(chunks):
        pl.when(has_up)(up_copies[c].wait_send)
        pl.when(has_down)(down_copies[c].wait_send)
    average, spread = exchange_end(copies2, st2)
    scale = g2v[...] * lax.rsqrt(spread + epsilon)
    shift = b2v[...]

    total = jnp.zeros((1, mid), f32)
    hidden = []
    for r in range(rows):
        h = jnp.maximum((middle[r] - average) * scale + shift, 0.0).astype(bf16)
        total = total + colsum(h.astype(f32))
        hidden.append(h)
    rest = total / count
    pieces = []
    for _ in range(3):
        piece = rest.astype(bf16).astype(f32)
        rest = rest - piece
        pieces.append(piece)
    pieces = jnp.concatenate(pieces + [jnp.zeros((13, mid), f32)], axis=0)
    pivot = colsum(dot(pieces.astype(bf16), we[...]))
    two = jnp.zeros((1, ch), f32)
    for r in range(rows):
        value = dot(hidden[r], we[...])
        last_out[:, r] = value.reshape(imgs, wid, ch)
        gap = value - pivot
        two = two + colsum(gap * gap)
    st3[0, 0:1, :] = pivot
    st3[0, 1:2, :] = two
    copies3 = exchange_start(2, st3)
    for copy in copies2:
        copy.wait_send()
    average, spread = exchange_end(copies3, st3)
    coef[0:1, :] = average
    coef[1:2, :] = g3v[...] * lax.rsqrt(spread + epsilon)
    for copy in copies3:
        copy.wait_send()


def finish(pieces, last, held, coef, b3, out, done, sem):
    rows = last.shape[0] // pieces
    scale = coef[1:2, :]
    mean = coef[0:1, :]
    shift = b3[...]
    copies = []
    for i in range(pieces):
        here = pl.ds(i * rows, rows)
        value = (last[here, :] - mean) * scale + shift + held[here, :].astype(f32)
        done[here, :] = jnp.maximum(value, 0.0).astype(bf16)
        copy = pltpu.make_async_copy(done.at[here], out.at[here], sem.at[i])
        copy.start()
        copies.append(copy)
    for copy in copies:
        copy.wait()


def body(images, w_reduce, w_spatial, w_expand, g1, b1, g2, b2, g3, b3):
    n = lax.axis_size(AXIS)
    imgs, rows, wid, ch = images.shape
    mid = w_reduce.shape[1]
    cells = imgs * wid
    chunks = [imgs // 2, imgs - imgs // 2] if imgs > 1 else [imgs]
    hbm = pl.BlockSpec(memory_space=pltpu.HBM)
    vmem = pl.BlockSpec(memory_space=pltpu.VMEM)
    vec = lambda c: pltpu.VMEM((1, c), f32)
    rowvec = lambda v: v.reshape(1, v.shape[0])
    halo = pltpu.VMEM((cells + PIVOT_ROWS, mid), bf16)
    held, last, coef = pl.pallas_call(
        functools.partial(kernel, n, imgs, rows, wid, chunks),
        out_shape=(
            jax.ShapeDtypeStruct(images.shape, bf16),
            jax.ShapeDtypeStruct(images.shape, f32),
            jax.ShapeDtypeStruct((2, ch), f32),
        ),
        in_specs=[hbm] * 9,
        out_specs=(vmem, vmem, vmem),
        scratch_shapes=[
            pltpu.VMEM((ch, mid), bf16),
            pltpu.VMEM((3, 3 * mid, mid), bf16),
            pltpu.VMEM((mid, ch), bf16),
            vec(mid), vec(mid), vec(mid), vec(mid), vec(ch),
            pltpu.VMEM((rows, cells, mid), f32),
            pltpu.VMEM((rows + 2, cells, 3 * mid), bf16),
            pltpu.VMEM((rows, cells, mid), f32),
            halo, halo, halo, halo,
            pltpu.VMEM((n, 2, mid), f32),
            pltpu.VMEM((n, 2, mid), f32),
            pltpu.VMEM((n, 2, ch), f32),
            pltpu.SemaphoreType.DMA((rows + 8,)),
            pltpu.SemaphoreType.DMA((2, len(chunks))),
            pltpu.SemaphoreType.DMA((2, len(chunks))),
            pltpu.SemaphoreType.DMA((3, n - 1)),
            pltpu.SemaphoreType.DMA((3, n - 1)),
        ],
        compiler_params=pltpu.CompilerParams(
            collective_id=0, has_side_effects=True, vmem_limit_bytes=32 * 1024 * 1024
        ),
        name="block_front",
    )(*[
        pltpu.with_memory_space_constraint(v, pltpu.HBM)
        for v in (
            images, w_reduce, w_spatial.reshape(3, 3 * mid, mid), w_expand,
            rowvec(g1), rowvec(b1), rowvec(g2), rowvec(b2), rowvec(g3),
        )
    ])
    total = imgs * rows * wid
    pieces = PIECES if total % (PIECES * 16) == 0 else 1
    out = pl.pallas_call(
        functools.partial(finish, pieces),
        out_shape=jax.ShapeDtypeStruct((total, ch), bf16),
        in_specs=[vmem] * 4,
        out_specs=hbm,
        scratch_shapes=[pltpu.VMEM((total, ch), bf16), pltpu.SemaphoreType.DMA((pieces,))],
        compiler_params=pltpu.CompilerParams(vmem_limit_bytes=16 * 1024 * 1024),
        name="block_finish",
    )(last.reshape(total, ch), held.reshape(total, ch), coef, rowvec(b3))
    return out.reshape(images.shape)


def solution(mesh):
    placed = (P("grp", "bn", None, None), P(), P(), P(), P(), P(), P(), P(), P(), P())
    return jax.shard_map(
        body, mesh=mesh, in_specs=placed, out_specs=P("grp", "bn", None, None), check_vma=False
    )
```

```python
import functools

import jax
import jax.numpy as jnp
from jax import lax
from jax.experimental import pallas as pl
from jax.experimental.pallas import tpu as pltpu
from jax.sharding import PartitionSpec as P

epsilon = 1e-05
AXIS = "bn"
f32 = jnp.float32
bf16 = jnp.bfloat16
PIVOT_ROWS = 16
PIECES = 8


def dot(a, b):
    return jnp.dot(a, b, preferred_element_type=f32)


def flipped(me, k):
    bit, out = 1, me
    while bit <= k:
        if k & bit:
            out = out + bit * (1 - 2 * lax.rem(me // bit, 2))
        bit *= 2
    return out


def kernel(
    n, imgs, rows, wid, chunks,
    images, w_reduce, w_spatial, w_expand, g1, b1, g2, b2, g3,
    x_out, last_out, coef,
    wr, ws, we, g1v, b1v, g2v, b2v, g3v,
    first, xcat, middle, up_src, down_src, up_dst, down_dst,
    st1, st2, st3,
    load_sem, halo_send, halo_recv, st_send, st_recv,
):
    me = lax.axis_index(AXIS)
    cells = imgs * wid
    sizes = [c * wid for c in chunks]
    starts = [sum(sizes[:c]) for c in range(len(sizes))]
    chunks = len(sizes)
    count = rows * cells
    mid = wr.shape[1]
    ch = wr.shape[0]
    paired = n & (n - 1) == 0

    def peer(k):
        return flipped(me, k) if paired else lax.rem(me + k, n)

    hops = list(range(n - 1, 0, -1))
    barrier = pltpu.get_barrier_semaphore()
    for k in hops:
        pl.semaphore_signal(
            barrier, inc=1, device_id={AXIS: peer(k)}, device_id_type=pl.DeviceIdType.MESH
        )

    edges = [0] + ([rows - 1] if rows > 1 else [])
    inner = [r for r in range(rows) if r not in edges]
    slot = iter(range(load_sem.shape[0]))

    def load(src, dst):
        copy = pltpu.make_async_copy(src, dst, load_sem.at[next(slot)])
        copy.start()
        return copy

    wr_copy = load(w_reduce, wr)
    x_copies = {r: load(images.at[:, r], x_out.at[:, r]) for r in edges + inner}
    first_vec = [load(g1, g1v), load(b1, b1v)]
    ws_copy = load(w_spatial, ws)
    mid_vec = [load(g2, g2v), load(b2, b2v)]
    we_copy = load(w_expand, we)
    last_vec = [load(g3, g3v)]

    has_up = me > 0
    has_down = me < n - 1

    def span(c):
        begin = 0 if c == 0 else PIVOT_ROWS + starts[c]
        return pl.ds(begin, PIVOT_ROWS + starts[c] + sizes[c] - begin)

    def halo_copy(c, side):
        src, dst, to = ((up_src, up_dst, n - 1), (down_src, down_dst, 1))[side]
        return pltpu.make_async_remote_copy(
            src_ref=src.at[span(c)], dst_ref=dst.at[span(c)],
            send_sem=halo_send.at[side, c], recv_sem=halo_recv.at[side, c],
            device_id={AXIS: lax.rem(me + to, n)}, device_id_type=pl.DeviceIdType.MESH,
        )

    up_copies = [halo_copy(c, 0) for c in range(chunks)]
    down_copies = [halo_copy(c, 1) for c in range(chunks)]

    def exchange_start(index, buf):
        copies = []
        for k in hops:
            copy = pltpu.make_async_remote_copy(
                src_ref=buf.at[0], dst_ref=buf.at[k],
                send_sem=st_send.at[index, k - 1], recv_sem=st_recv.at[index, k - 1],
                device_id={AXIS: peer(k)}, device_id_type=pl.DeviceIdType.MESH,
            )
            copy.start()
            copies.append(copy)
        return copies

    def exchange_end(copies, buf):
        for copy in copies:
            copy.wait_recv()
        values = buf[...]
        total = jnp.sum(values, axis=0)
        average = total[0:1] / n
        gap = values[:, 0:1, :] - average
        spread = (total[1:2] + count * jnp.sum(gap * gap, axis=0)) / (n * count)
        return average, spread

    def colsum(v):
        return jnp.sum(v, axis=0, keepdims=True)

    def pooled(buf, pivot, one, two):
        buf[0, 0:1, :] = pivot + one / count
        buf[0, 1:2, :] = two - one * (one / count)

    wr_copy.wait()
    pivot = None
    one = jnp.zeros((1, mid), f32)
    two = jnp.zeros((1, mid), f32)
    for r in edges + inner:
        if r == (edges + inner)[-1]:
            pl.semaphore_wait(barrier, n - 1)
            pl.when(has_up)(up_copies[0].start)
            pl.when(has_down)(down_copies[0].start)
        x_copies[r].wait()
        value = dot(x_out[:, r].reshape(cells, ch), wr[...])
        first[r] = value
        if pivot is None:
            pivot = colsum(value) / cells
        gap = value - pivot
        one = one + colsum(gap)
        two = two + colsum(gap * gap)
        for row, src in ((0, up_src), (rows - 1, down_src)):
            if r == row:
                centre = (colsum(value) / cells).astype(bf16)
                sent = (value - centre.astype(f32)).astype(bf16)
                src[pl.ds(0, PIVOT_ROWS), :] = jnp.broadcast_to(centre, (PIVOT_ROWS, mid))
                src[pl.ds(PIVOT_ROWS, cells), :] = sent
    pooled(st1, pivot, one, two)

    copies1 = exchange_start(0, st1)
    for c in range(1, chunks):
        pl.when(has_up)(up_copies[c].start)
        pl.when(has_down)(down_copies[c].start)

    for copy in first_vec:
        copy.wait()
    average, spread = exchange_end(copies1, st1)
    scale = g1v[...] * lax.rsqrt(spread + epsilon)
    shift = b1v[...]

    def columns(size):
        shape = (size // wid, wid, mid)
        return lax.broadcasted_iota(jnp.int32, shape, 1).reshape(size, mid)

    def fill(r, start, value):
        size = value.shape[0]
        column = columns(size)
        h = jnp.maximum((value - average) * scale + shift, 0.0)
        here = pl.ds(start, size)
        xcat[r, here, pl.ds(mid, mid)] = h.astype(bf16)
        before = jnp.where(column == 0, 0.0, pltpu.roll(h, 1, 0))
        xcat[r, here, pl.ds(0, mid)] = before.astype(bf16)
        after = jnp.where(column == wid - 1, 0.0, pltpu.roll(h, size - 1, 0))
        xcat[r, here, pl.ds(2 * mid, mid)] = after.astype(bf16)

    for r in range(rows):
        fill(r + 1, 0, first[r])

    ws_copy.wait()
    for r in range(rows):
        acc = dot(xcat[r + 1], ws[1])
        if r > 0:
            acc = acc + dot(xcat[r], ws[0])
        if r < rows - 1:
            acc = acc + dot(xcat[r + 2], ws[2])
        middle[r] = acc

    based = inner or edges
    pivot = jnp.zeros((1, mid), f32)
    for r in based:
        pivot = pivot + colsum(middle[r])
    pivot = pivot / (len(based) * cells)
    one = jnp.zeros((1, mid), f32)
    two = jnp.zeros((1, mid), f32)
    for r in inner:
        gap = middle[r] - pivot
        one = one + colsum(gap)
        two = two + colsum(gap * gap)

    def add_halo(dst, c, padded_row, row, tap):
        value = dst[pl.ds(PIVOT_ROWS + starts[c], sizes[c]), :].astype(f32)
        fill(padded_row, starts[c], value + dst[pl.ds(0, 1), :].astype(f32))
        here = pl.ds(starts[c], sizes[c])
        middle[row, here, :] += dot(xcat[padded_row, here, :], ws[tap])

    for c in range(chunks):
        @pl.when(has_down)
        def _():
            up_copies[c].wait_recv()
            add_halo(up_dst, c, rows + 1, rows - 1, 2)

        @pl.when(has_up)
        def _():
            down_copies[c].wait_recv()
            add_halo(down_dst, c, 0, 0, 0)

        for r in edges:
            gap = middle[r, pl.ds(starts[c], sizes[c]), :] - pivot
            one = one + colsum(gap)
            two = two + colsum(gap * gap)

    pooled(st2, pivot, one, two)
    copies2 = exchange_start(1, st2)
    for copy in mid_vec + last_vec:
        copy.wait()
    we_copy.wait()
    for copy in copies1:
        copy.wait_send()
    for c in range(chunks):
        pl.when(has_up)(up_copies[c].wait_send)
        pl.when(has_down)(down_copies[c].wait_send)
    average, spread = exchange_end(copies2, st2)
    scale = g2v[...] * lax.rsqrt(spread + epsilon)
    shift = b2v[...]

    total = jnp.zeros((1, mid), f32)
    hidden = []
    for r in range(rows):
        h = jnp.maximum((middle[r] - average) * scale + shift, 0.0).astype(bf16)
        total = total + colsum(h.astype(f32))
        hidden.append(h)
    rest = total / count
    pieces = []
    for _ in range(3):
        piece = rest.astype(bf16).astype(f32)
        rest = rest - piece
        pieces.append(piece)
    pieces = jnp.concatenate(pieces + [jnp.zeros((13, mid), f32)], axis=0)
    pivot = colsum(dot(pieces.astype(bf16), we[...]))
    two = jnp.zeros((1, ch), f32)
    for r in range(rows):
        value = dot(hidden[r], we[...])
        last_out[:, r] = value.reshape(imgs, wid, ch)
        gap = value - pivot
        two = two + colsum(gap * gap)
    st3[0, 0:1, :] = pivot
    st3[0, 1:2, :] = two
    copies3 = exchange_start(2, st3)
    for copy in copies2:
        copy.wait_send()
    average, spread = exchange_end(copies3, st3)
    coef[0:1, :] = average
    coef[1:2, :] = g3v[...] * lax.rsqrt(spread + epsilon)
    for copy in copies3:
        copy.wait_send()


def finish(pieces, last, held, coef, b3, out, done, sem):
    rows = last.shape[0] // pieces
    scale = coef[1:2, :]
    mean = coef[0:1, :]
    shift = b3[...]
    copies = []
    for i in range(pieces):
        here = pl.ds(i * rows, rows)
        value = (last[here, :] - mean) * scale + shift + held[here, :].astype(f32)
        done[here, :] = jnp.maximum(value, 0.0).astype(bf16)
        copy = pltpu.make_async_copy(done.at[here], out.at[here], sem.at[i])
        copy.start()
        copies.append(copy)
    for copy in copies:
        copy.wait()


def body(images, w_reduce, w_spatial, w_expand, g1, b1, g2, b2, g3, b3):
    n = lax.axis_size(AXIS)
    imgs, rows, wid, ch = images.shape
    mid = w_reduce.shape[1]
    cells = imgs * wid
    chunks = [1, imgs - 1] if imgs > 1 else [imgs]
    hbm = pl.BlockSpec(memory_space=pltpu.HBM)
    vmem = pl.BlockSpec(memory_space=pltpu.VMEM)
    vec = lambda c: pltpu.VMEM((1, c), f32)
    rowvec = lambda v: v.reshape(1, v.shape[0])
    halo = pltpu.VMEM((cells + PIVOT_ROWS, mid), bf16)
    held, last, coef = pl.pallas_call(
        functools.partial(kernel, n, imgs, rows, wid, chunks),
        out_shape=(
            jax.ShapeDtypeStruct(images.shape, bf16),
            jax.ShapeDtypeStruct(images.shape, f32),
            jax.ShapeDtypeStruct((2, ch), f32),
        ),
        in_specs=[hbm] * 9,
        out_specs=(vmem, vmem, vmem),
        scratch_shapes=[
            pltpu.VMEM((ch, mid), bf16),
            pltpu.VMEM((3, 3 * mid, mid), bf16),
            pltpu.VMEM((mid, ch), bf16),
            vec(mid), vec(mid), vec(mid), vec(mid), vec(ch),
            pltpu.VMEM((rows, cells, mid), f32),
            pltpu.VMEM((rows + 2, cells, 3 * mid), bf16),
            pltpu.VMEM((rows, cells, mid), f32),
            halo, halo, halo, halo,
            pltpu.VMEM((n, 2, mid), f32),
            pltpu.VMEM((n, 2, mid), f32),
            pltpu.VMEM((n, 2, ch), f32),
            pltpu.SemaphoreType.DMA((rows + 8,)),
            pltpu.SemaphoreType.DMA((2, len(chunks))),
            pltpu.SemaphoreType.DMA((2, len(chunks))),
            pltpu.SemaphoreType.DMA((3, n - 1)),
            pltpu.SemaphoreType.DMA((3, n - 1)),
        ],
        compiler_params=pltpu.CompilerParams(
            collective_id=0, has_side_effects=True, vmem_limit_bytes=32 * 1024 * 1024
        ),
        name="block_front",
    )(*[
        pltpu.with_memory_space_constraint(v, pltpu.HBM)
        for v in (
            images, w_reduce, w_spatial.reshape(3, 3 * mid, mid), w_expand,
            rowvec(g1), rowvec(b1), rowvec(g2), rowvec(b2), rowvec(g3),
        )
    ])
    total = imgs * rows * wid
    pieces = PIECES if total % (PIECES * 16) == 0 else 1
    out = pl.pallas_call(
        functools.partial(finish, pieces),
        out_shape=jax.ShapeDtypeStruct((total, ch), bf16),
        in_specs=[vmem] * 4,
        out_specs=hbm,
        scratch_shapes=[pltpu.VMEM((total, ch), bf16), pltpu.SemaphoreType.DMA((pieces,))],
        compiler_params=pltpu.CompilerParams(vmem_limit_bytes=16 * 1024 * 1024),
        name="block_finish",
    )(last.reshape(total, ch), held.reshape(total, ch), coef, rowvec(b3))
    return out.reshape(images.shape)


def solution(mesh):
    placed = (P("grp", "bn", None, None), P(), P(), P(), P(), P(), P(), P(), P(), P())
    return jax.shard_map(
        body, mesh=mesh, in_specs=placed, out_specs=P("grp", "bn", None, None), check_vma=False
    )
```
